32 devices in a mesh: ep: 4 (over y, x), fsdp: 8 (over z, core).
Axes of the slice: x: 2, y: 2, z: 4, core: 2. Of those that a mesh axis runs over, the one named last changes fastest.
Arguments:
- w_gate: float32 [64, 2048, 1024], P('ep', 'fsdp'), may hold values from -0.1875 to 0.1875
- avg_gate: bfloat16 [64, 2048, 1024], P('ep', 'fsdp'), may hold values from -0.0625 to 0.0625
- w_up: float32 [64, 2048, 1024], P('ep', 'fsdp'), may hold values from -0.1875 to 0.1875
- avg_up: bfloat16 [64, 2048, 1024], P('ep', 'fsdp'), may hold values from -0.0625 to 0.0625
- w_down: float32 [64, 1024, 2048], P('ep', None, 'fsdp'), may hold values from -0.25 to 0.25
- avg_down: bfloat16 [64, 1024, 2048], P('ep', None, 'fsdp'), may hold values from -0.09375 to 0.09375
- router_weight: float32 [2048, 64], P('fsdp', 'ep'), may hold values from -0.125 to 0.125
- router_gain: float32 [2048], P('fsdp'), may hold values from 0.25 to 1.75
Outputs:
- serve_gate: bfloat16 [64, 2048, 1024], P('ep', None, 'fsdp')
- serve_up: bfloat16 [64, 2048, 1024], P('ep', None, 'fsdp')
- serve_down: bfloat16 [64, 1024, 2048], P('ep', 'fsdp')
- scale_gate: float32 [64, 1024], P('ep', 'fsdp')
- scale_up: float32 [64, 1024], P('ep', 'fsdp')
- scale_down: float32 [64, 1024], P('ep', 'fsdp')
- serve_router: bfloat16 [2048, 64], replicated
The draws below stay inside these ranges and needn't reach their ends.
All inputs are finite; a program needn't handle non-finite values.
Results may differ from the reference program's by a relative error of at most 0.001.
Values may be sent and summed in bfloat16 or wider, within the bound.
A program may use at most 192 MiB of HBM per device.

```python
import jax
import jax.numpy as jnp
from jax import lax

EXPERTS = 64
D_MODEL = 2048
D_EXPERT = 1024


def with_spikes(result, stream_key, source, target, blocks, factor):
    owner, partner = [(jnp.arange(result.shape[axis_at]) // (result.shape[axis_at] // blocks)).reshape([-1 if axis == axis_at else 1 for axis in range(result.ndim)]) for axis_at in (source, target)]
    chosen = jax.random.permutation(stream_key, blocks)[partner]
    strong = (owner == chosen) | (owner == (partner + blocks // 2) % blocks)
    return jnp.where(strong, factor * result, result)


def levels(rng, shape, split, least, top_value):
    gain, own = 1.0, jax.random.fold_in(rng, 6)
    for position, shards_of in split:
        steps = jnp.exp(jax.random.uniform(jax.random.fold_in(own, position), (shards_of,), jnp.float32, least / len(split), top_value / len(split)))
        gain = gain * jnp.repeat(steps, shape[position] // shards_of).reshape([-1 if axis == position else 1 for axis in range(len(shape))])
    return gain


def centred(rng, dims, width, bound, cuts=(), kind=jnp.bfloat16):
    drawn = jax.random.normal(rng, dims, jnp.float32) * width
    if len(cuts) > 0:
        drawn = levels(rng, dims, cuts, -0.22, 0.18) * drawn
    return jnp.clip(drawn, min=-bound, max=bound).astype(kind)


def gaussian_with(stream_key, shape, spread, reach, split, heavy, dtype=jnp.bfloat16):
    values = spread * jax.random.normal(stream_key, shape, jnp.float32)
    if split:
        values = values * levels(stream_key, shape, split, -0.22, 0.18)
    return jnp.clip(with_spikes(values, jax.random.fold_in(stream_key, 3), *heavy), -reach, reach).astype(dtype)


def setup_inputs(seed: int = 0) -> dict:
    splits = jax.random.split(jax.random.key(seed), 9)
    w_gate = gaussian_with(splits[0], (EXPERTS, D_MODEL, D_EXPERT), D_MODEL ** -0.5, 0.1875, ((0, 4), (1, 8)), (1, 2, 8, 2.0), jnp.float32)
    avg_gate = centred(splits[1], (EXPERTS, D_MODEL, D_EXPERT), (D_MODEL * 4) ** -0.5, 0.0625, ((0, 4), (1, 8)))
    w_up = gaussian_with(splits[2], (EXPERTS, D_MODEL, D_EXPERT), D_MODEL ** -0.5, 0.1875, ((0, 4), (1, 8)), (1, 2, 8, 2.0), jnp.float32)
    avg_up = centred(splits[3], (EXPERTS, D_MODEL, D_EXPERT), (D_MODEL * 4) ** -0.5, 0.0625, ((0, 4), (1, 8)))
    w_down = gaussian_with(splits[4], (EXPERTS, D_EXPERT, D_MODEL), D_EXPERT ** -0.5, 0.25, ((0, 4), (2, 8)), (2, 1, 8, 2.0), jnp.float32)
    avg_down = centred(splits[5], (EXPERTS, D_EXPERT, D_MODEL), (D_EXPERT * 4) ** -0.5, 0.09375, ((0, 4), (2, 8)))
    router_weight = centred(splits[6], (D_MODEL, EXPERTS), D_MODEL ** -0.5, 0.125, ((0, 8), (1, 4)), jnp.float32)
    router_gain = jnp.clip(1.0 + 0.15 * jax.random.normal(splits[7], (D_MODEL,), jnp.float32), 0.25, 1.75)
    return {"w_gate": w_gate, "avg_gate": avg_gate, "w_up": w_up, "avg_up": avg_up, "w_down": w_down, "avg_down": avg_down, "router_weight": router_weight, "router_gain": router_gain}


def reference(w_gate, avg_gate, w_up, avg_up, w_down, avg_down, router_weight, router_gain):
    fresh_gate = w_gate + avg_gate.astype(jnp.float32)
    fresh_up = w_up + avg_up.astype(jnp.float32)
    fresh_down = w_down + avg_down.astype(jnp.float32)
    scale_gate = jnp.sqrt(lax.optimization_barrier(jnp.sum(fresh_gate * fresh_gate, axis=1)))
    serve_gate = (fresh_gate / jnp.expand_dims(scale_gate, 1)).astype(jnp.bfloat16)
    scale_up = jnp.sqrt(lax.optimization_barrier(jnp.sum(fresh_up * fresh_up, axis=1)))
    serve_up = (fresh_up / jnp.expand_dims(scale_up, 1)).astype(jnp.bfloat16)
    scale_down = jnp.sqrt(lax.optimization_barrier(jnp.sum(fresh_down * fresh_down, axis=2)))
    serve_down = (fresh_down / jnp.expand_dims(scale_down, 2)).astype(jnp.bfloat16)
    serve_router = (router_weight * router_gain[:, None]).astype(jnp.bfloat16)
    return (serve_gate, serve_up, serve_down, scale_gate, scale_up, scale_down, serve_router)
```

```python
import functools

import jax
import jax.numpy as jnp
from jax import lax
from jax.experimental import pallas as pl
from jax.experimental.pallas import tpu as pltpu
from jax.sharding import PartitionSpec as P

MESH = pl.DeviceIdType.MESH
MIB = 1 << 20
SLOTS = 4
RING = 8
LANES = 128


def chunks_of(experts):
    first = max(1, experts // 8)
    early = max(first, experts // 2)
    return first, early


def fresh_of(w, avg):
    return w + avg.astype(jnp.float32)


def work_kernel(
    wg_ref, ag_ref, wu_ref, au_ref, wd_ref, ad_ref, rw_ref, gain_ref,
    og_ref, ou_ref, od_ref, scale_ref, router_ref,
    wide_w, wide_avg, tall_w, tall_avg, wide_stage, tall_stage,
    part_a, part_b, part_c, sums_a, sums_b, sums_c, inv_a, inv_b, inv_c, own_router,
    wide_sem, tall_sem, wide_sent, tall_sent, landed,
    sums_sent, sums_landed, inv_sent, inv_landed, router_sent, router_landed,
):
    n, ep = lax.axis_size("fsdp"), lax.axis_size("ep")
    me, group = lax.axis_index("fsdp"), lax.axis_index("ep")
    experts, depth, d_expert = wg_ref.shape
    width = d_expert // n
    first, early = chunks_of(experts)

    barrier = pltpu.get_barrier_semaphore()
    for d in range(1, n):
        pl.semaphore_signal(
            barrier, inc=1, device_id={"fsdp": lax.rem(me + d, n)}, device_id_type=MESH
        )
    for d in range(1, ep):
        pl.semaphore_signal(
            barrier, inc=1, device_id={"ep": lax.rem(group + d, ep)}, device_id_type=MESH
        )

    gate = (wg_ref, ag_ref, wide_w, wide_avg, wide_sem)
    up = (wu_ref, au_ref, wide_w, wide_avg, wide_sem)
    down = (wd_ref, ad_ref, tall_w, tall_avg, tall_sem)

    def loads(m, e, slot):
        w, avg, w_buf, avg_buf, sem = m
        return (
            pltpu.make_async_copy(w.at[e], w_buf.at[slot], sem.at[slot, 0]),
            pltpu.make_async_copy(avg.at[e], avg_buf.at[slot], sem.at[slot, 1]),
        )

    def prime(m, start, stop):
        for i in range(min(SLOTS, stop - start)):
            for copy in loads(m, start + i, i):
                copy.start()

    def stream(m, start, stop, body):
        count = stop - start

        def step(i, carry):
            slot = lax.rem(i, SLOTS)
            for copy in loads(m, start + i, slot):
                copy.wait()
            body(start + i, slot)

            @pl.when(i + SLOTS < count)
            def _():
                for copy in loads(m, start + i + SLOTS, slot):
                    copy.start()

            return carry

        lax.fori_loop(0, count, step, 0)

    def column_sums(part, shift, e, slot):
        for k in range(n):
            at = slice(k * width, (k + 1) * width)
            fresh = fresh_of(wide_w[slot, :, at], wide_avg[slot, :, at])
            part[k, pl.ds(e + shift, 1), :] = jnp.sum(fresh * fresh, axis=0, keepdims=True)

    def row_sums(part, shift, e, slot):
        span = tall_w.shape[2]
        for k in range(n):
            at = slice(k * width, (k + 1) * width)
            total = None
            for c in range(span // LANES):
                lanes = slice(c * LANES, (c + 1) * LANES)
                fresh = fresh_of(tall_w[slot, at, lanes], tall_avg[slot, at, lanes])
                total = fresh * fresh if total is None else total + fresh * fresh
            part[k, pl.ds(e + shift, 1), :] = jnp.sum(total.T, axis=0, keepdims=True)

    def to_all(send):
        for d in range(1, n):
            send(lax.rem(me + d, n))

    def send_sums(chunk, part, sums):
        sums[me] = part[me]

        def send(k):
            pltpu.make_async_remote_copy(
                src_ref=part.at[k], dst_ref=sums.at[me],
                send_sem=sums_sent.at[chunk], recv_sem=sums_landed.at[chunk],
                device_id={"fsdp": k}, device_id_type=MESH,
            ).start()

        to_all(send)

    def others(ref, sem):
        some = ref.at[pl.ds(0, n - 1)]
        return pltpu.make_async_copy(some, some, sem)

    def send_inverse(chunk, sums, inv, places):
        others(sums, sums_landed.at[chunk]).wait()
        total = sums[0]
        for k in range(1, n):
            total = total + sums[k]
        scale = jnp.sqrt(total)
        at = 0
        for m, start, stop in places:
            scale_ref[m, start:stop] = scale[at : at + stop - start]
            at += stop - start
        inv[me] = 1.0 / scale

        def send(k):
            pltpu.make_async_remote_copy(
                src_ref=inv.at[me], dst_ref=inv.at[me],
                send_sem=inv_sent.at[chunk], recv_sem=inv_landed.at[chunk],
                device_id={"fsdp": k}, device_id_type=MESH,
            ).start()

        to_all(send)

    def ring_slot(stage, sent, count):
        ring = lax.rem(count, RING)

        @pl.when(count >= RING)
        def _():
            others(stage.at[ring], sent.at[ring]).wait()

        return ring

    def wide_pieces(m, out, inv, shift, e, slot):
        ring = ring_slot(wide_stage, wide_sent, m * experts + e)
        for k in range(n):
            at = slice(k * width, (k + 1) * width)
            fresh = fresh_of(wide_w[slot, :, at], wide_avg[slot, :, at])
            wide_stage[ring, k] = (fresh * inv[k, pl.ds(e + shift, 1), :]).astype(jnp.bfloat16)
        rows = pl.ds(pl.multiple_of(me * depth, depth), depth)

        def send(k):
            pltpu.make_async_remote_copy(
                src_ref=wide_stage.at[ring, k], dst_ref=out.at[e, rows],
                send_sem=wide_sent.at[ring], recv_sem=landed.at[m, e],
                device_id={"fsdp": k}, device_id_type=MESH,
            ).start()

        to_all(send)
        out[e, rows] = wide_stage[ring, me]

    def tall_pieces(inv, shift, e, slot):
        ring = ring_slot(tall_stage, tall_sent, e)
        span = tall_w.shape[2]
        for k in range(n):
            at = slice(k * width, (k + 1) * width)
            row = inv[k, pl.ds(e + shift, 1), :]
            factor = jnp.broadcast_to(row, (LANES, width)).T
            for c in range(span // LANES):
                lanes = slice(c * LANES, (c + 1) * LANES)
                fresh = fresh_of(tall_w[slot, at, lanes], tall_avg[slot, at, lanes])
                tall_stage[ring, k, :, lanes] = (fresh * factor).astype(jnp.bfloat16)
        columns = pl.ds(pl.multiple_of(me * span, span), span)

        def send(k):
            pltpu.make_async_remote_copy(
                src_ref=tall_stage.at[ring, k], dst_ref=od_ref.at[e, :, columns],
                send_sem=tall_sent.at[ring], recv_sem=landed.at[2, e],
                device_id={"fsdp": k}, device_id_type=MESH,
            ).start()

        to_all(send)
        od_ref[e, :, columns] = tall_stage[ring, me]

    prime(gate, 0, first)
    own_router[...] = (rw_ref[...] * gain_ref[...]).astype(jnp.bfloat16)
    pl.semaphore_wait(barrier, n - 1 + ep - 1)

    stream(gate, 0, first, functools.partial(column_sums, part_a, 0))
    prime(gate, first, early)
    send_sums(0, part_a, sums_a)
    stream(gate, first, early, functools.partial(column_sums, part_b, -first))
    prime(gate, 0, first)
    send_sums(1, part_b, sums_b)
    send_inverse(0, sums_a, inv_a, ((0, 0, first),))

    my_columns = pl.ds(pl.multiple_of(me * depth, depth), depth)

    def send_router(k):
        pltpu.make_async_remote_copy(
            src_ref=own_router, dst_ref=router_ref.at[group, :, my_columns],
            send_sem=router_sent.at[0], recv_sem=router_landed.at[0],
            device_id={"fsdp": k}, device_id_type=MESH,
        ).start()

    def router_wait(sem):
        some = router_ref.at[group, :, pl.ds(0, (n - 1) * depth)]
        return pltpu.make_async_copy(some, some, sem)

    send_inverse(1, sums_b, inv_b, ((0, first, early),))
    others(inv_a, inv_landed.at[0]).wait()
    stream(gate, 0, first, functools.partial(wide_pieces, 0, og_ref, inv_a, 0))
    pieces_b = functools.partial(wide_pieces, 0, og_ref, inv_b, -first)
    cut_one = first + (early - first + 2) // 3
    cut_two = cut_one + (early - cut_one + 1) // 2
    prime(gate, first, cut_one)
    others(inv_b, inv_landed.at[1]).wait()
    stream(gate, first, cut_one, pieces_b)
    to_all(send_router)
    router_ref[group, :, my_columns] = own_router[...]

    prime(gate, early, experts)
    prime(down, 0, experts)
    stream(gate, early, experts, functools.partial(column_sums, part_c, -early))
    rest = experts - early
    prime(up, 0, experts)
    stream(up, 0, experts, functools.partial(column_sums, part_c, rest))
    stream(down, 0, experts, functools.partial(row_sums, part_c, rest + experts))
    send_sums(2, part_c, sums_c)
    prime(gate, cut_one, cut_two)
    stream(gate, cut_one, cut_two, pieces_b)

    router_wait(router_landed.at[0]).wait()
    for d in range(1, ep):
        pltpu.make_async_remote_copy(
            src_ref=router_ref.at[group], dst_ref=router_ref.at[group],
            send_sem=router_sent.at[1], recv_sem=router_landed.at[1],
            device_id={"ep": lax.rem(group + d, ep)}, device_id_type=MESH,
        ).start()

    send_inverse(
        2, sums_c, inv_c, ((0, early, experts), (1, 0, experts), (2, 0, experts))
    )
    prime(gate, cut_two, early)
    stream(gate, cut_two, early, pieces_b)
    prime(gate, early, experts)
    prime(down, 0, experts)
    others(inv_c, inv_landed.at[2]).wait()
    stream(gate, early, experts, functools.partial(wide_pieces, 0, og_ref, inv_c, -early))
    prime(up, 0, experts)
    stream(up, 0, experts, functools.partial(wide_pieces, 1, ou_ref, inv_c, rest))
    stream(down, 0, experts, functools.partial(tall_pieces, inv_c, rest + experts))

    def finish(e, carry):
        wide = wide_stage.at[0, pl.ds(0, n - 1)]
        tall = tall_stage.at[0, pl.ds(0, n - 1)]
        for m, some in ((0, wide), (1, wide), (2, tall)):
            pltpu.make_async_copy(some, some, landed.at[m, e]).wait()
        return carry

    lax.fori_loop(0, experts, finish, 0)

    def drain(count, stage, sent):
        def step(i, carry):
            others(stage.at[i], sent.at[i]).wait()
            return carry

        lax.fori_loop(0, min(RING, count), step, 0)

    drain(2 * experts, wide_stage, wide_sent)
    drain(experts, tall_stage, tall_sent)
    for chunk, (part, inv) in enumerate(((part_a, inv_a), (part_b, inv_b), (part_c, inv_c))):
        others(part, sums_sent.at[chunk]).wait()
        others(inv, inv_sent.at[chunk]).wait()
    router_wait(router_sent.at[0]).wait()
    if ep > 1:
        some = router_ref.at[pl.ds(0, ep - 1)]
        pltpu.make_async_copy(some, some, router_sent.at[1]).wait()
        pltpu.make_async_copy(some, some, router_landed.at[1]).wait()


def write_kernel(
    g_ref, u_ref, d_ref, scale_ref, router_ref,
    og_ref, ou_ref, od_ref, sg_ref, su_ref, sd_ref, out_router_ref, big, small,
):
    copies = []
    experts = g_ref.shape[0]
    parts = min(4, experts)
    span = experts // parts
    for m, (src, dst) in enumerate(((g_ref, og_ref), (u_ref, ou_ref), (d_ref, od_ref))):
        for i in range(parts):
            at = pl.ds(i * span, span)
            copies.append(pltpu.make_async_copy(src.at[at], dst.at[at], big.at[m, i]))
    for m, dst in enumerate((sg_ref, su_ref, sd_ref)):
        copies.append(pltpu.make_async_copy(scale_ref.at[m], dst, small.at[m]))
    copies.append(pltpu.make_async_copy(router_ref, out_router_ref, small.at[3]))
    for copy in copies:
        copy.start()
    for copy in copies:
        copy.wait()


def on_device(w_gate, avg_gate, w_up, avg_up, w_down, avg_down, router_weight, router_gain):
    n, ep = lax.axis_size("fsdp"), lax.axis_size("ep")
    experts, depth, d_expert = w_gate.shape
    span = w_down.shape[2]
    width = d_expert // n
    first, early = chunks_of(experts)
    rows = router_weight.shape[1]
    f32, bf16 = jnp.float32, jnp.bfloat16
    hbm = pl.BlockSpec(memory_space=pl.ANY)
    vmem = pl.BlockSpec(memory_space=pltpu.VMEM)
    shapes = (
        ((experts, n * depth, width), bf16),
        ((experts, n * depth, width), bf16),
        ((experts, width, n * span), bf16),
        ((3, experts, width), f32),
        ((ep, rows, n * depth), bf16),
    )
    counts = (first, early - first, 3 * experts - early)
    dma = pltpu.SemaphoreType.DMA
    work = pl.pallas_call(
        work_kernel,
        out_shape=[pltpu.VMEM(*shape) for shape in shapes],
        in_specs=[hbm] * 6 + [vmem] * 2,
        out_specs=[vmem] * 5,
        scratch_shapes=[
            pltpu.VMEM((SLOTS, depth, d_expert), f32),
            pltpu.VMEM((SLOTS, depth, d_expert), bf16),
            pltpu.VMEM((SLOTS, d_expert, span), f32),
            pltpu.VMEM((SLOTS, d_expert, span), bf16),
            pltpu.VMEM((RING, n, depth, width), bf16),
            pltpu.VMEM((RING, n, width, span), bf16),
            *[pltpu.VMEM((n, count, width), f32) for _ in range(3) for count in counts],
            pltpu.VMEM((rows, depth), bf16),
            dma((SLOTS, 2)),
            dma((SLOTS, 2)),
            dma((RING,)),
            dma((RING,)),
            dma((3, experts)),
            *[dma((3,)) for _ in range(4)],
            dma((2,)),
            dma((2,)),
        ],
        compiler_params=pltpu.CompilerParams(
            collective_id=0, has_side_effects=True, vmem_limit_bytes=30 * MIB
        ),
    )
    results = work(
        w_gate, avg_gate, w_up, avg_up, w_down, avg_down,
        router_weight.T, router_gain.reshape(1, depth),
    )
    outs = (
        shapes[0],
        shapes[1],
        shapes[2],
        ((experts, width), f32),
        ((experts, width), f32),
        ((experts, width), f32),
        shapes[4],
    )
    write = pl.pallas_call(
        write_kernel,
        out_shape=[jax.ShapeDtypeStruct(*shape) for shape in outs],
        in_specs=[vmem] * 5,
        out_specs=[hbm] * 7,
        scratch_shapes=[dma((3, min(4, experts))), dma((4,))],
        compiler_params=pltpu.CompilerParams(vmem_limit_bytes=4 * MIB),
    )
    *arrays, router = write(*results)
    return (*arrays, router.reshape(ep * rows, n * depth).T)


def solution(mesh):
    placed = (
        P("ep", "fsdp", None),
        P("ep", "fsdp", None),
        P("ep", "fsdp", None),
        P("ep", "fsdp", None),
        P("ep", None, "fsdp"),
        P("ep", None, "fsdp"),
        P("fsdp", "ep"),
        P("fsdp"),
    )
    return jax.shard_map(
        on_device,
        mesh=mesh,
        in_specs=placed,
        out_specs=(
            P("ep", None, "fsdp"),
            P("ep", None, "fsdp"),
            P("ep", "fsdp", None),
            P("ep", "fsdp"),
            P("ep", "fsdp"),
            P("ep", "fsdp"),
            P(),
        ),
        check_vma=False,
    )
```

```python
import functools

import jax
import jax.numpy as jnp
from jax import lax
from jax.experimental import pallas as pl
from jax.experimental.pallas import tpu as pltpu
from jax.sharding import PartitionSpec as P

MESH = pl.DeviceIdType.MESH
MIB = 1 << 20
SLOTS = 4
RING = 8
LANES = 128


def chunks_of(experts):
    first = max(1, experts // 8)
    early = max(first, experts // 2)
    return first, early


def place_of(k, n):
    return (k % 2) * (n // 2) + k // 2


def fresh_of(w, avg):
    return w + avg.astype(jnp.float32)


def work_kernel(
    wg_ref, ag_ref, wu_ref, au_ref, wd_ref, ad_ref, rw_ref, gain_ref,
    og_ref, ou_ref, od_ref, scale_ref, router_ref,
    wide_w, wide_avg, tall_w, tall_avg, wide_stage, tall_stage,
    part_a, part_b, part_c, sums_a, sums_b, sums_c, inv_a, inv_b, inv_c, pair_c, own_router,
    wide_sem, tall_sem, wide_sent, tall_sent, landed,
    sums_sent, sums_landed, inv_sent, inv_landed, pair_sent, pair_landed,
    router_sent, router_landed,
):
    n, ep = lax.axis_size("fsdp"), lax.axis_size("ep")
    me, group = lax.axis_index("fsdp"), lax.axis_index("ep")
    experts, depth, d_expert = wg_ref.shape
    width = d_expert // n
    first, early = chunks_of(experts)
    half = n // 2
    core, chip = lax.rem(me, 2), me // 2
    place = core * half + chip

    barrier = pltpu.get_barrier_semaphore()
    for d in range(1, n):
        pl.semaphore_signal(
            barrier, inc=1, device_id={"fsdp": lax.rem(me + d, n)}, device_id_type=MESH
        )
    for d in range(1, ep):
        pl.semaphore_signal(
            barrier, inc=1, device_id={"ep": lax.rem(group + d, ep)}, device_id_type=MESH
        )

    gate = (wg_ref, ag_ref, wide_w, wide_avg, wide_sem)
    up = (wu_ref, au_ref, wide_w, wide_avg, wide_sem)
    down = (wd_ref, ad_ref, tall_w, tall_avg, tall_sem)

    def loads(m, e, slot):
        w, avg, w_buf, avg_buf, sem = m
        return (
            pltpu.make_async_copy(w.at[e], w_buf.at[slot], sem.at[slot, 0]),
            pltpu.make_async_copy(avg.at[e], avg_buf.at[slot], sem.at[slot, 1]),
        )

    def prime(m, start, stop):
        for i in range(min(SLOTS, stop - start)):
            for copy in loads(m, start + i, i):
                copy.start()

    def stream(m, start, stop, body):
        count = stop - start

        def step(i, carry):
            slot = lax.rem(i, SLOTS)
            for copy in loads(m, start + i, slot):
                copy.wait()
            body(start + i, slot)

            @pl.when(i + SLOTS < count)
            def _():
                for copy in loads(m, start + i + SLOTS, slot):
                    copy.start()

            return carry

        lax.fori_loop(0, count, step, 0)

    def column_sums(part, shift, e, slot):
        for k in range(n):
            at = slice(k * width, (k + 1) * width)
            fresh = fresh_of(wide_w[slot, :, at], wide_avg[slot, :, at])
            part[place_of(k, n), pl.ds(e + shift, 1), :] = jnp.sum(fresh * fresh, axis=0, keepdims=True)

    def row_sums(part, shift, e, slot):
        span = tall_w.shape[2]
        for k in range(n):
            at = slice(k * width, (k + 1) * width)
            total = None
            for c in range(span // LANES):
                lanes = slice(c * LANES, (c + 1) * LANES)
                fresh = fresh_of(tall_w[slot, at, lanes], tall_avg[slot, at, lanes])
                total = fresh * fresh if total is None else total + fresh * fresh
            part[place_of(k, n), pl.ds(e + shift, 1), :] = jnp.sum(total.T, axis=0, keepdims=True)

    def to_all(send):
        for d in range(1, n):
            send(lax.rem(me + d, n))

    def others(ref, sem, count=n - 1):
        some = ref.at[pl.ds(0, count)]
        return pltpu.make_async_copy(some, some, sem)

    def remote(src, dst, sent, arrived, k):
        return pltpu.make_async_remote_copy(
            src_ref=src, dst_ref=dst, send_sem=sent, recv_sem=arrived,
            device_id={"fsdp": k}, device_id_type=MESH,
        )

    def send_first():
        sums_a[me] = part_a[...]
        to_all(
            lambda k: remote(
                part_a, sums_a.at[me], sums_sent.at[0], sums_landed.at[0], k
            ).start()
        )

    def take_first():
        others(sums_a, sums_landed.at[0]).wait()

        def total(of):
            result = of(0)
            for k in range(1, n):
                result = result + of(k)
            return result

        scale_ref[0, 0:first] = jnp.sqrt(total(lambda k: sums_a[k, place]))
        inv_a[...] = 1.0 / jnp.sqrt(total(lambda k: sums_a[k]))

    def send_early():
        sums_b[me] = part_b[place]

        def send(k):
            at = lax.rem(k, 2) * half + k // 2
            remote(part_b.at[at], sums_b.at[me], sums_sent.at[1], sums_landed.at[1], k).start()

        to_all(send)

    def keep_scale(scale, places):
        at = 0
        for m, start, stop in places:
            scale_ref[m, start:stop] = scale[at : at + stop - start]
            at += stop - start

    def send_early_inverse():
        others(sums_b, sums_landed.at[1]).wait()
        total = sums_b[0]
        for k in range(1, n):
            total = total + sums_b[k]
        scale = jnp.sqrt(total)
        keep_scale(scale, ((0, first, early),))
        inv_b[place] = 1.0 / scale
        to_all(
            lambda k: remote(
                inv_b.at[place], inv_b.at[place], inv_sent.at[1], inv_landed.at[1], k
            ).start()
        )

    def to_chips(send):
        for d in range(1, half):
            z = lax.rem(chip + d, half)
            send(z, z * 2 + core)

    sibling = me + 1 - 2 * core
    theirs = pl.ds(pl.multiple_of((1 - core) * half, half), half)
    ours = pl.ds(pl.multiple_of(core * half, half), half)

    def send_rest():
        copy = remote(part_c.at[theirs], pair_c, pair_sent.at[0], pair_landed.at[0], sibling)
        copy.start()
        copy.wait_recv()
        part_c[ours] = part_c[ours] + pair_c[...]
        sums_c[chip] = part_c[place]

        def send(z, k):
            remote(
                part_c.at[core * half + z], sums_c.at[chip],
                sums_sent.at[2], sums_landed.at[2], k,
            ).start()

        to_chips(send)

    def send_rest_inverse(places):
        if half > 1:
            others(sums_c, sums_landed.at[2], half - 1).wait()
        total = sums_c[0]
        for z in range(1, half):
            total = total + sums_c[z]
        scale = jnp.sqrt(total)
        keep_scale(scale, places)
        inv_c[place] = 1.0 / scale
        to_chips(
            lambda z, k: remote(
                inv_c.at[place], inv_c.at[place], inv_sent.at[2], inv_landed.at[2], k
            ).start()
        )

    def share_rest_inverse():
        if half > 1:
            others(inv_c, inv_landed.at[2], half - 1).wait()
        copy = remote(inv_c.at[ours], inv_c.at[ours], pair_sent.at[1], pair_landed.at[1], sibling)
        copy.start()
        copy.wait_recv()

    def ring_slot(stage, sent, count):
        ring = lax.rem(count, RING)

        @pl.when(count >= RING)
        def _():
            others(stage.at[ring], sent.at[ring]).wait()

        return ring

    def wide_pieces(m, out, inv, shift, e, slot):
        ring = ring_slot(wide_stage, wide_sent, m * experts + e)
        for k in range(n):
            at = slice(k * width, (k + 1) * width)
            fresh = fresh_of(wide_w[slot, :, at], wide_avg[slot, :, at])
            wide_stage[ring, k] = (fresh * inv[place_of(k, n), pl.ds(e + shift, 1), :]).astype(jnp.bfloat16)
        rows = pl.ds(pl.multiple_of(me * depth, depth), depth)

        def send(k):
            pltpu.make_async_remote_copy(
                src_ref=wide_stage.at[ring, k], dst_ref=out.at[e, rows],
                send_sem=wide_sent.at[ring], recv_sem=landed.at[m, e],
                device_id={"fsdp": k}, device_id_type=MESH,
            ).start()

        to_all(send)
        out[e, rows] = wide_stage[ring, me]

    def tall_pieces(inv, shift, e, slot):
        ring = ring_slot(tall_stage, tall_sent, e)
        span = tall_w.shape[2]
        for k in range(n):
            at = slice(k * width, (k + 1) * width)
            row = inv[place_of(k, n), pl.ds(e + shift, 1), :]
            factor = jnp.broadcast_to(row, (LANES, width)).T
            for c in range(span // LANES):
                lanes = slice(c * LANES, (c + 1) * LANES)
                fresh = fresh_of(tall_w[slot, at, lanes], tall_avg[slot, at, lanes])
                tall_stage[ring, k, :, lanes] = (fresh * factor).astype(jnp.bfloat16)
        columns = pl.ds(pl.multiple_of(me * span, span), span)

        def send(k):
            pltpu.make_async_remote_copy(
                src_ref=tall_stage.at[ring, k], dst_ref=od_ref.at[e, :, columns],
                send_sem=tall_sent.at[ring], recv_sem=landed.at[2, e],
                device_id={"fsdp": k}, device_id_type=MESH,
            ).start()

        to_all(send)
        od_ref[e, :, columns] = tall_stage[ring, me]

    my_columns = pl.ds(pl.multiple_of(me * depth, depth), depth)

    def router_wait(sem):
        some = router_ref.at[group, :, pl.ds(0, (n - 1) * depth)]
        return pltpu.make_async_copy(some, some, sem)

    for e in range(first):
        for copy in loads(gate, e, SLOTS + e):
            copy.start()
    own_router[...] = (rw_ref[...] * gain_ref[...]).astype(jnp.bfloat16)
    router_ref[group, :, my_columns] = own_router[...]
    for e in range(first):
        for copy in loads(gate, e, SLOTS + e):
            copy.wait()
    prime(gate, first, early)
    for e in range(first):
        column_sums(part_a, 0, e, SLOTS + e)
    pl.semaphore_wait(barrier, n - 1 + ep - 1)
    send_first()
    stream(gate, first, early, functools.partial(column_sums, part_b, -first))
    send_early()
    to_all(
        lambda k: remote(
            own_router, router_ref.at[group, :, my_columns],
            router_sent.at[0], router_landed.at[0], k,
        ).start()
    )
    prime(gate, early, experts)
    prime(down, 0, experts)

    take_first()
    wide_pieces(0, og_ref, inv_a, 0, 0, SLOTS)
    send_early_inverse()
    for e in range(1, first):
        wide_pieces(0, og_ref, inv_a, 0, e, SLOTS + e)

    rest = experts - early
    stream(gate, early, experts, functools.partial(column_sums, part_c, -early))
    prime(up, 0, experts)
    stream(up, 0, experts, functools.partial(column_sums, part_c, rest))

    pieces_b = functools.partial(wide_pieces, 0, og_ref, inv_b, -first)
    cut_one = first + (early - first + 1) // 2
    cut_two = cut_one + (early - cut_one + 1) // 2
    prime(gate, first, cut_one)
    others(inv_b, inv_landed.at[1]).wait()
    stream(gate, first, cut_one, pieces_b)

    stream(down, 0, experts, functools.partial(row_sums, part_c, rest + experts))
    prime(gate, cut_one, cut_two)
    send_rest()
    stream(gate, cut_one, cut_two, pieces_b)

    router_wait(router_landed.at[0]).wait()
    for d in range(1, ep):
        pltpu.make_async_remote_copy(
            src_ref=router_ref.at[group], dst_ref=router_ref.at[group],
            send_sem=router_sent.at[1], recv_sem=router_landed.at[1],
            device_id={"ep": lax.rem(group + d, ep)}, device_id_type=MESH,
        ).start()

    prime(gate, cut_two, early)
    send_rest_inverse(((0, early, experts), (1, 0, experts), (2, 0, experts)))
    stream(gate, cut_two, early, pieces_b)
    prime(gate, early, experts)
    prime(down, 0, experts)
    share_rest_inverse()
    stream(gate, early, experts, functools.partial(wide_pieces, 0, og_ref, inv_c, -early))
    prime(up, 0, experts)
    stream(up, 0, experts, functools.partial(wide_pieces, 1, ou_ref, inv_c, rest))
    stream(down, 0, experts, functools.partial(tall_pieces, inv_c, rest + experts))

    def arrived(m, e):
        stage = tall_stage if m == 2 else wide_stage
        others(stage.at[0], landed.at[m, e]).wait()

    def finish(m):
        def step(e, carry):
            arrived(m, e)
            return carry

        lax.fori_loop(0, experts, step, 0)

    def drain(count, stage, sent):
        def step(i, carry):
            others(stage.at[i], sent.at[i]).wait()
            return carry

        lax.fori_loop(0, min(RING, count), step, 0)

    others(sums_a, sums_sent.at[0]).wait()
    others(part_b, sums_sent.at[1]).wait()
    others(inv_b, inv_sent.at[1]).wait()
    if half > 1:
        others(sums_c, sums_sent.at[2], half - 1).wait()
        others(inv_c, inv_sent.at[2], half - 1).wait()
    others(pair_c, pair_sent.at[0], half).wait()
    others(inv_c, pair_sent.at[1], half).wait()
    router_wait(router_sent.at[0]).wait()
    if ep > 1:
        some = router_ref.at[pl.ds(0, ep - 1)]
        pltpu.make_async_copy(some, some, router_sent.at[1]).wait()
        pltpu.make_async_copy(some, some, router_landed.at[1]).wait()
    finish(0)
    finish(1)
    drain(2 * experts, wide_stage, wide_sent)
    drain(experts, tall_stage, tall_sent)
    finish(2)


def write_kernel(
    g_ref, u_ref, d_ref, scale_ref, router_ref,
    og_ref, ou_ref, od_ref, sg_ref, su_ref, sd_ref, out_router_ref, big, small,
):
    copies = []
    experts = g_ref.shape[0]
    parts = min(4, experts)
    span = experts // parts
    for m, (src, dst) in enumerate(((g_ref, og_ref), (u_ref, ou_ref), (d_ref, od_ref))):
        for i in range(parts):
            at = pl.ds(i * span, span)
            copies.append(pltpu.make_async_copy(src.at[at], dst.at[at], big.at[m, i]))
    for m, dst in enumerate((sg_ref, su_ref, sd_ref)):
        copies.append(pltpu.make_async_copy(scale_ref.at[m], dst, small.at[m]))
    copies.append(pltpu.make_async_copy(router_ref, out_router_ref, small.at[3]))
    for copy in copies:
        copy.start()
    for copy in copies:
        copy.wait()


def on_device(w_gate, avg_gate, w_up, avg_up, w_down, avg_down, router_weight, router_gain):
    n, ep = lax.axis_size("fsdp"), lax.axis_size("ep")
    experts, depth, d_expert = w_gate.shape
    span = w_down.shape[2]
    width = d_expert // n
    first, early = chunks_of(experts)
    rows = router_weight.shape[1]
    f32, bf16 = jnp.float32, jnp.bfloat16
    hbm = pl.BlockSpec(memory_space=pl.ANY)
    vmem = pl.BlockSpec(memory_space=pltpu.VMEM)
    shapes = (
        ((experts, n * depth, width), bf16),
        ((experts, n * depth, width), bf16),
        ((experts, width, n * span), bf16),
        ((3, experts, width), f32),
        ((ep, rows, n * depth), bf16),
    )
    counts = (first, early - first, 3 * experts - early)
    dma = pltpu.SemaphoreType.DMA
    work = pl.pallas_call(
        work_kernel,
        out_shape=[pltpu.VMEM(*shape) for shape in shapes],
        in_specs=[hbm] * 6 + [vmem] * 2,
        out_specs=[vmem] * 5,
        scratch_shapes=[
            pltpu.VMEM((SLOTS + first, depth, d_expert), f32),
            pltpu.VMEM((SLOTS + first, depth, d_expert), bf16),
            pltpu.VMEM((SLOTS, d_expert, span), f32),
            pltpu.VMEM((SLOTS, d_expert, span), bf16),
            pltpu.VMEM((RING, n, depth, width), bf16),
            pltpu.VMEM((RING, n, width, span), bf16),
            *[pltpu.VMEM((n, count, width), f32) for count in counts],
            pltpu.VMEM((n, n, first, width), f32),
            pltpu.VMEM((n, counts[1], width), f32),
            pltpu.VMEM((n // 2, counts[2], width), f32),
            *[pltpu.VMEM((n, count, width), f32) for count in counts],
            pltpu.VMEM((n // 2, counts[2], width), f32),
            pltpu.VMEM((rows, depth), bf16),
            dma((SLOTS + first, 2)),
            dma((SLOTS, 2)),
            dma((RING,)),
            dma((RING,)),
            dma((3, experts)),
            *[dma((3,)) for _ in range(4)],
            *[dma((2,)) for _ in range(4)],
        ],
        compiler_params=pltpu.CompilerParams(
            collective_id=0, has_side_effects=True, vmem_limit_bytes=30 * MIB
        ),
    )
    results = work(
        w_gate, avg_gate, w_up, avg_up, w_down, avg_down,
        router_weight.T, router_gain.reshape(1, depth),
    )
    outs = (
        shapes[0],
        shapes[1],
        shapes[2],
        ((experts, width), f32),
        ((experts, width), f32),
        ((experts, width), f32),
        shapes[4],
    )
    write = pl.pallas_call(
        write_kernel,
        out_shape=[jax.ShapeDtypeStruct(*shape) for shape in outs],
        in_specs=[vmem] * 5,
        out_specs=[hbm] * 7,
        scratch_shapes=[dma((3, min(4, experts))), dma((4,))],
        compiler_params=pltpu.CompilerParams(vmem_limit_bytes=4 * MIB),
    )
    *arrays, router = write(*results)
    return (*arrays, router.reshape(ep * rows, n * depth).T)


def solution(mesh):
    placed = (
        P("ep", "fsdp", None),
        P("ep", "fsdp", None),
        P("ep", "fsdp", None),
        P("ep", "fsdp", None),
        P("ep", None, "fsdp"),
        P("ep", None, "fsdp"),
        P("fsdp", "ep"),
        P("fsdp"),
    )
    return jax.shard_map(
        on_device,
        mesh=mesh,
        in_specs=placed,
        out_specs=(
            P("ep", None, "fsdp"),
            P("ep", None, "fsdp"),
            P("ep", "fsdp", None),
            P("ep", "fsdp"),
            P("ep", "fsdp"),
            P("ep", "fsdp"),
            P(),
        ),
        check_vma=False,
    )
```

```python
import functools

import jax
import jax.numpy as jnp
from jax import lax
from jax.experimental import pallas as pl
from jax.experimental.pallas import tpu as pltpu
from jax.sharding import PartitionSpec as P

MESH = pl.DeviceIdType.MESH
MIB = 1 << 20
SLOTS = 4
RING = 8
LANES = 128


def chunks_of(experts):
    first = max(1, experts // 8)
    early = max(first + 1, experts * 3 // 8)
    return first, early


def place_of(k, n):
    chip, place, width = k // 2, 0, n // 2
    while width > 1:
        width //= 2
        place = place + (chip % 2) * width
        chip = chip // 2
    return (k % 2) * (n // 2) + place


def fresh_of(w, avg):
    return w + avg.astype(jnp.float32)


def work_kernel(
    wg_ref, ag_ref, wu_ref, au_ref, wd_ref, ad_ref, rw_ref, gain_ref,
    og_ref, ou_ref, od_ref, scale_ref, router_ref,
    wide_w, wide_avg, tall_w, tall_avg, wide_stage, tall_stage,
    part_a, part_b, part_c, sums_a, sums_b, sums_c, inv_a, inv_b, inv_c, pair_c, own_router,
    wide_sem, tall_sem, wide_sent, tall_sent, landed,
    sums_sent, sums_landed, inv_sent, inv_landed, pair_sent, pair_landed,
    router_sent, router_landed,
):
    n, ep = lax.axis_size("fsdp"), lax.axis_size("ep")
    me, group = lax.axis_index("fsdp"), lax.axis_index("ep")
    experts, depth, d_expert = wg_ref.shape
    width = d_expert // n
    first, early = chunks_of(experts)
    half = n // 2
    core, chip = lax.rem(me, 2), me // 2
    place = place_of(me, n)
    steps = half.bit_length() - 1

    barrier = pltpu.get_barrier_semaphore()
    for d in range(1, n):
        pl.semaphore_signal(
            barrier, inc=1, device_id={"fsdp": lax.rem(me + d, n)}, device_id_type=MESH
        )
    for d in range(1, ep):
        pl.semaphore_signal(
            barrier, inc=1, device_id={"ep": lax.rem(group + d, ep)}, device_id_type=MESH
        )

    gate = (wg_ref, ag_ref, wide_w, wide_avg, wide_sem)
    up = (wu_ref, au_ref, wide_w, wide_avg, wide_sem)
    down = (wd_ref, ad_ref, tall_w, tall_avg, tall_sem)

    def loads(m, e, slot):
        w, avg, w_buf, avg_buf, sem = m
        return (
            pltpu.make_async_copy(w.at[e], w_buf.at[slot], sem.at[slot, 0]),
            pltpu.make_async_copy(avg.at[e], avg_buf.at[slot], sem.at[slot, 1]),
        )

    def prime(m, start, stop):
        for i in range(min(SLOTS, stop - start)):
            for copy in loads(m, start + i, i):
                copy.start()

    def stream(m, start, stop, body):
        count = stop - start

        def step(i, carry):
            slot = lax.rem(i, SLOTS)
            for copy in loads(m, start + i, slot):
                copy.wait()
            body(start + i, slot)

            @pl.when(i + SLOTS < count)
            def _():
                for copy in loads(m, start + i + SLOTS, slot):
                    copy.start()

            return carry

        lax.fori_loop(0, count, step, 0)

    def column_sums(part, shift, e, slot):
        for k in range(n):
            at = slice(k * width, (k + 1) * width)
            fresh = fresh_of(wide_w[slot, :, at], wide_avg[slot, :, at])
            part[place_of(k, n), pl.ds(e + shift, 1), :] = jnp.sum(fresh * fresh, axis=0, keepdims=True)

    def row_sums(part, shift, e, slot):
        span = tall_w.shape[2]
        for k in range(n):
            at = slice(k * width, (k + 1) * width)
            total = None
            for c in range(span // LANES):
                lanes = slice(c * LANES, (c + 1) * LANES)
                fresh = fresh_of(tall_w[slot, at, lanes], tall_avg[slot, at, lanes])
                total = fresh * fresh if total is None else total + fresh * fresh
            part[place_of(k, n), pl.ds(e + shift, 1), :] = jnp.sum(total.T, axis=0, keepdims=True)

    def to_all(send):
        for d in range(1, n):
            send(lax.rem(me + d, n))

    def others(ref, sem, count=n - 1):
        some = ref.at[pl.ds(0, count)]
        return pltpu.make_async_copy(some, some, sem)

    def remote(src, dst, sent, arrived, k):
        return pltpu.make_async_remote_copy(
            src_ref=src, dst_ref=dst, send_sem=sent, recv_sem=arrived,
            device_id={"fsdp": k}, device_id_type=MESH,
        )

    def send_first():
        sums_a[me] = part_a[...]
        to_all(
            lambda k: remote(
                part_a, sums_a.at[me], sums_sent.at[0], sums_landed.at[0], k
            ).start()
        )

    def take_first():
        others(sums_a, sums_landed.at[0]).wait()

        def total(of):
            result = of(0)
            for k in range(1, n):
                result = result + of(k)
            return result

        scale_ref[0, 0:first] = jnp.sqrt(total(lambda k: sums_a[k, place]))
        inv_a[...] = 1.0 / jnp.sqrt(total(lambda k: sums_a[k]))

    def send_early():
        sums_b[me] = part_b[place]

        def send(k):
            remote(part_b.at[place_of(k, n)], sums_b.at[me], sums_sent.at[1], sums_landed.at[1], k).start()

        to_all(send)

    def keep_scale(scale, places):
        at = 0
        for m, start, stop in places:
            scale_ref[m, start:stop] = scale[at : at + stop - start]
            at += stop - start

    def send_early_inverse():
        others(sums_b, sums_landed.at[1]).wait()
        total = sums_b[0]
        for k in range(1, n):
            total = total + sums_b[k]
        scale = jnp.sqrt(total)
        keep_scale(scale, ((0, first, early),))
        inv_b[place] = 1.0 / scale
        to_all(
            lambda k: remote(
                inv_b.at[place], inv_b.at[place], inv_sent.at[1], inv_landed.at[1], k
            ).start()
        )

    def across(step):
        bit = chip // (1 << step) % 2
        return bit, (chip + (1 - 2 * bit) * (1 << step)) * 2 + core

    sibling = me + 1 - 2 * core
    theirs = pl.ds(pl.multiple_of((1 - core) * half, half), half)
    ours = pl.ds(pl.multiple_of(core * half, half), half)

    def send_rest():
        copy = remote(part_c.at[theirs], pair_c, pair_sent.at[0], pair_landed.at[0], sibling)
        copy.start()
        copy.wait_recv()
        part_c[ours] = part_c[ours] + pair_c[...]

    def halving(step):
        size = half >> (step + 1)
        base = core * half
        for before in range(step):
            base = base + across(before)[0] * (half >> (before + 1))
        bit, partner = across(step)
        keep, give = base + bit * size, base + (1 - bit) * size
        inbox = pl.ds(half - 2 * size, size)
        copy = remote(
            part_c.at[pl.ds(give, size)], sums_c.at[inbox],
            sums_sent.at[2 + step], sums_landed.at[2 + step], partner,
        )
        return copy, pl.ds(keep, size), inbox

    def send_half(step):
        halving(step)[0].start()

    def take_half(step):
        copy, keep, inbox = halving(step)
        copy.wait_recv()
        part_c[keep] = part_c[keep] + sums_c[inbox]

    def make_rest_inverse(places):
        scale = jnp.sqrt(part_c[place])
        keep_scale(scale, places)
        inv_c[place] = 1.0 / scale

    def doubling(step):
        size = half >> (step + 1)
        base = core * half
        for before in range(step + 1):
            base = base + across(before)[0] * (half >> (before + 1))
        some = inv_c.at[pl.ds(base, size)]
        return remote(
            some, some, inv_sent.at[2 + step], inv_landed.at[2 + step], across(step)[1]
        )

    def share_rest_inverse():
        copy = remote(inv_c.at[ours], inv_c.at[ours], pair_sent.at[1], pair_landed.at[1], sibling)
        copy.start()
        copy.wait_recv()

    def ring_slot(stage, sent, count):
        ring = lax.rem(count, RING)

        @pl.when(count >= RING)
        def _():
            others(stage.at[ring], sent.at[ring]).wait()

        return ring

    def wide_pieces(m, out, inv, shift, e, slot):
        ring = ring_slot(wide_stage, wide_sent, m * experts + e)
        for k in range(n):
            at = slice(k * width, (k + 1) * width)
            fresh = fresh_of(wide_w[slot, :, at], wide_avg[slot, :, at])
            wide_stage[ring, k] = (fresh * inv[place_of(k, n), pl.ds(e + shift, 1), :]).astype(jnp.bfloat16)
        rows = pl.ds(pl.multiple_of(me * depth, depth), depth)

        def send(k):
            pltpu.make_async_remote_copy(
                src_ref=wide_stage.at[ring, k], dst_ref=out.at[e, rows],
                send_sem=wide_sent.at[ring], recv_sem=landed.at[m, e],
                device_id={"fsdp": k}, device_id_type=MESH,
            ).start()

        to_all(send)
        out[e, rows] = wide_stage[ring, me]

    def tall_pieces(inv, shift, e, slot):
        ring = ring_slot(tall_stage, tall_sent, e)
        span = tall_w.shape[2]
        for k in range(n):
            at = slice(k * width, (k + 1) * width)
            row = inv[place_of(k, n), pl.ds(e + shift, 1), :]
            factor = jnp.broadcast_to(row, (LANES, width)).T
            for c in range(span // LANES):
                lanes = slice(c * LANES, (c + 1) * LANES)
                fresh = fresh_of(tall_w[slot, at, lanes], tall_avg[slot, at, lanes])
                tall_stage[ring, k, :, lanes] = (fresh * factor).astype(jnp.bfloat16)
        columns = pl.ds(pl.multiple_of(me * span, span), span)

        def send(k):
            pltpu.make_async_remote_copy(
                src_ref=tall_stage.at[ring, k], dst_ref=od_ref.at[e, :, columns],
                send_sem=tall_sent.at[ring], recv_sem=landed.at[2, e],
                device_id={"fsdp": k}, device_id_type=MESH,
            ).start()

        to_all(send)
        od_ref[e, :, columns] = tall_stage[ring, me]

    my_columns = pl.ds(pl.multiple_of(me * depth, depth), depth)

    def router_wait(sem):
        some = router_ref.at[group, :, pl.ds(0, (n - 1) * depth)]
        return pltpu.make_async_copy(some, some, sem)

    for e in range(first):
        for copy in loads(gate, e, SLOTS + e):
            copy.start()
    own_router[...] = (rw_ref[...] * gain_ref[...]).astype(jnp.bfloat16)
    router_ref[group, :, my_columns] = own_router[...]
    for e in range(first):
        for copy in loads(gate, e, SLOTS + e):
            copy.wait()
    prime(gate, first, early)
    for e in range(first):
        column_sums(part_a, 0, e, SLOTS + e)
    pl.semaphore_wait(barrier, n - 1 + ep - 1)
    send_first()
    stream(gate, first, early, functools.partial(column_sums, part_b, -first))
    send_early()
    to_all(
        lambda k: remote(
            own_router, router_ref.at[group, :, my_columns],
            router_sent.at[0], router_landed.at[0], k,
        ).start()
    )
    prime(gate, early, experts)
    prime(down, 0, experts)

    take_first()
    wide_pieces(0, og_ref, inv_a, 0, 0, SLOTS)
    send_early_inverse()
    for e in range(1, first):
        wide_pieces(0, og_ref, inv_a, 0, e, SLOTS + e)

    rest = experts - early
    stream(gate, early, experts, functools.partial(column_sums, part_c, -early))
    prime(up, 0, experts)
    stream(up, 0, experts, functools.partial(column_sums, part_c, rest))

    pieces_b = functools.partial(wide_pieces, 0, og_ref, inv_b, -first)
    cut_one = first + (early - first + 1) // 2
    prime(gate, first, cut_one)
    others(inv_b, inv_landed.at[1]).wait()
    stream(gate, first, cut_one, pieces_b)

    stream(down, 0, experts, functools.partial(row_sums, part_c, rest + experts))
    send_rest()
    turns = 2 * steps
    cuts = [cut_one + (early - cut_one) * i // max(1, turns) for i in range(turns + 1)]
    for step in range(steps):
        send_half(step)
        prime(gate, cuts[step], cuts[step + 1])
        stream(gate, cuts[step], cuts[step + 1], pieces_b)
        take_half(step)
    make_rest_inverse(((0, early, experts), (1, 0, experts), (2, 0, experts)))

    router_wait(router_landed.at[0]).wait()
    for d in range(1, ep):
        pltpu.make_async_remote_copy(
            src_ref=router_ref.at[group], dst_ref=router_ref.at[group],
            send_sem=router_sent.at[1], recv_sem=router_landed.at[1],
            device_id={"ep": lax.rem(group + d, ep)}, device_id_type=MESH,
        ).start()

    for turn, step in enumerate(reversed(range(steps)), steps):
        doubling(step).start()
        prime(gate, cuts[turn], cuts[turn + 1])
        stream(gate, cuts[turn], cuts[turn + 1], pieces_b)
        doubling(step).wait_recv()
    prime(gate, early, experts)
    prime(down, 0, experts)
    share_rest_inverse()
    stream(gate, early, experts, functools.partial(wide_pieces, 0, og_ref, inv_c, -early))
    prime(up, 0, experts)
    stream(up, 0, experts, functools.partial(wide_pieces, 1, ou_ref, inv_c, rest))
    stream(down, 0, experts, functools.partial(tall_pieces, inv_c, rest + experts))

    def arrived(m, e):
        stage = tall_stage if m == 2 else wide_stage
        others(stage.at[0], landed.at[m, e]).wait()

    def finish(m):
        def step(e, carry):
            arrived(m, e)
            return carry

        lax.fori_loop(0, experts, step, 0)

    def drain(count, stage, sent):
        def step(i, carry):
            others(stage.at[i], sent.at[i]).wait()
            return carry

        lax.fori_loop(0, min(RING, count), step, 0)

    others(sums_a, sums_sent.at[0]).wait()
    others(part_b, sums_sent.at[1]).wait()
    others(inv_b, inv_sent.at[1]).wait()
    for step in range(steps):
        halving(step)[0].wait_send()
        doubling(step).wait_send()
    others(pair_c, pair_sent.at[0], half).wait()
    others(inv_c, pair_sent.at[1], half).wait()
    router_wait(router_sent.at[0]).wait()
    if ep > 1:
        some = router_ref.at[pl.ds(0, ep - 1)]
        pltpu.make_async_copy(some, some, router_sent.at[1]).wait()
        pltpu.make_async_copy(some, some, router_landed.at[1]).wait()
    finish(0)
    finish(1)
    drain(2 * experts, wide_stage, wide_sent)
    drain(experts, tall_stage, tall_sent)
    finish(2)


def write_kernel(
    g_ref, u_ref, d_ref, scale_ref, router_ref,
    og_ref, ou_ref, od_ref, sg_ref, su_ref, sd_ref, out_router_ref, big, small,
):
    copies = []
    experts = g_ref.shape[0]
    parts = min(4, experts)
    span = experts // parts
    for m, (src, dst) in enumerate(((g_ref, og_ref), (u_ref, ou_ref), (d_ref, od_ref))):
        for i in range(parts):
            at = pl.ds(i * span, span)
            copies.append(pltpu.make_async_copy(src.at[at], dst.at[at], big.at[m, i]))
    for m, dst in enumerate((sg_ref, su_ref, sd_ref)):
        copies.append(pltpu.make_async_copy(scale_ref.at[m], dst, small.at[m]))
    copies.append(pltpu.make_async_copy(router_ref, out_router_ref, small.at[3]))
    for copy in copies:
        copy.start()
    for copy in copies:
        copy.wait()


def on_device(w_gate, avg_gate, w_up, avg_up, w_down, avg_down, router_weight, router_gain):
    n, ep = lax.axis_size("fsdp"), lax.axis_size("ep")
    experts, depth, d_expert = w_gate.shape
    span = w_down.shape[2]
    width = d_expert // n
    first, early = chunks_of(experts)
    rows = router_weight.shape[1]
    f32, bf16 = jnp.float32, jnp.bfloat16
    hbm = pl.BlockSpec(memory_space=pl.ANY)
    vmem = pl.BlockSpec(memory_space=pltpu.VMEM)
    shapes = (
        ((experts, n * depth, width), bf16),
        ((experts, n * depth, width), bf16),
        ((experts, width, n * span), bf16),
        ((3, experts, width), f32),
        ((ep, rows, n * depth), bf16),
    )
    counts = (first, early - first, 3 * experts - early)
    dma = pltpu.SemaphoreType.DMA
    work = pl.pallas_call(
        work_kernel,
        out_shape=[pltpu.VMEM(*shape) for shape in shapes],
        in_specs=[hbm] * 6 + [vmem] * 2,
        out_specs=[vmem] * 5,
        scratch_shapes=[
            pltpu.VMEM((SLOTS + first, depth, d_expert), f32),
            pltpu.VMEM((SLOTS + first, depth, d_expert), bf16),
            pltpu.VMEM((SLOTS, d_expert, span), f32),
            pltpu.VMEM((SLOTS, d_expert, span), bf16),
            pltpu.VMEM((RING, n, depth, width), bf16),
            pltpu.VMEM((RING, n, width, span), bf16),
            *[pltpu.VMEM((n, count, width), f32) for count in counts],
            pltpu.VMEM((n, n, first, width), f32),
            pltpu.VMEM((n, counts[1], width), f32),
            pltpu.VMEM((max(1, n // 2 - 1), counts[2], width), f32),
            *[pltpu.VMEM((n, count, width), f32) for count in counts],
            pltpu.VMEM((n // 2, counts[2], width), f32),
            pltpu.VMEM((rows, depth), bf16),
            dma((SLOTS + first, 2)),
            dma((SLOTS, 2)),
            dma((RING,)),
            dma((RING,)),
            dma((3, experts)),
            *[dma((2 + n.bit_length(),)) for _ in range(4)],
            *[dma((2,)) for _ in range(4)],
        ],
        compiler_params=pltpu.CompilerParams(
            collective_id=0, has_side_effects=True, vmem_limit_bytes=30 * MIB
        ),
    )
    results = work(
        w_gate, avg_gate, w_up, avg_up, w_down, avg_down,
        router_weight.T, router_gain.reshape(1, depth),
    )
    outs = (
        shapes[0],
        shapes[1],
        shapes[2],
        ((experts, width), f32),
        ((experts, width), f32),
        ((experts, width), f32),
        shapes[4],
    )
    write = pl.pallas_call(
        write_kernel,
        out_shape=[jax.ShapeDtypeStruct(*shape) for shape in outs],
        in_specs=[vmem] * 5,
        out_specs=[hbm] * 7,
        scratch_shapes=[dma((3, min(4, experts))), dma((4,))],
        compiler_params=pltpu.CompilerParams(vmem_limit_bytes=4 * MIB),
    )
    *arrays, router = write(*results)
    return (*arrays, router.reshape(ep * rows, n * depth).T)


def solution(mesh):
    placed = (
        P("ep", "fsdp", None),
        P("ep", "fsdp", None),
        P("ep", "fsdp", None),
        P("ep", "fsdp", None),
        P("ep", None, "fsdp"),
        P("ep", None, "fsdp"),
        P("fsdp", "ep"),
        P("fsdp"),
    )
    return jax.shard_map(
        on_device,
        mesh=mesh,
        in_specs=placed,
        out_specs=(
            P("ep", None, "fsdp"),
            P("ep", None, "fsdp"),
            P("ep", "fsdp", None),
            P("ep", "fsdp"),
            P("ep", "fsdp"),
            P("ep", "fsdp"),
            P(),
        ),
        check_vma=False,
    )
```

```python
import functools

import jax
import jax.numpy as jnp
from jax import lax
from jax.experimental import pallas as pl
from jax.experimental.pallas import tpu as pltpu
from jax.sharding import PartitionSpec as P

MESH = pl.DeviceIdType.MESH
MIB = 1 << 20
SLOTS = 4
RING = 8
LANES = 128


def chunks_of(experts):
    first = max(1, experts // 8)
    early = max(first + 1, experts * 3 // 8)
    return first, early


def place_of(k, n):
    chip, place, width = k // 2, 0, n // 2
    while width > 1:
        width //= 2
        place = place + (chip % 2) * width
        chip = chip // 2
    return (k % 2) * (n // 2) + place


def fresh_of(w, avg):
    return w + avg.astype(jnp.float32)


def work_kernel(
    wg_ref, ag_ref, wu_ref, au_ref, wd_ref, ad_ref, rw_ref, gain_ref,
    og_ref, ou_ref, od_ref, scale_ref, router_ref,
    wide_w, wide_avg, tall_w, tall_avg, wide_stage, tall_stage,
    part_a, part_b, part_c, sums_a, sums_b, sums_c, inv_a, inv_b, inv_c, pair_c, own_router,
    wide_sem, tall_sem, wide_sent, tall_sent, landed,
    sums_sent, sums_landed, inv_sent, inv_landed, pair_sent, pair_landed,
    router_sent, router_landed,
):
    n, ep = lax.axis_size("fsdp"), lax.axis_size("ep")
    me, group = lax.axis_index("fsdp"), lax.axis_index("ep")
    experts, depth, d_expert = wg_ref.shape
    width = d_expert // n
    first, early = chunks_of(experts)
    half = n // 2
    core, chip = lax.rem(me, 2), me // 2
    place = place_of(me, n)
    steps = half.bit_length() - 1

    barrier = pltpu.get_barrier_semaphore()
    for d in range(1, n):
        pl.semaphore_signal(
            barrier, inc=1, device_id={"fsdp": lax.rem(me + d, n)}, device_id_type=MESH
        )
    for d in range(1, ep):
        pl.semaphore_signal(
            barrier, inc=1, device_id={"ep": lax.rem(group + d, ep)}, device_id_type=MESH
        )

    gate = (wg_ref, ag_ref, wide_w, wide_avg, wide_sem)
    up = (wu_ref, au_ref, wide_w, wide_avg, wide_sem)
    down = (wd_ref, ad_ref, tall_w, tall_avg, tall_sem)

    def loads(m, e, slot):
        w, avg, w_buf, avg_buf, sem = m
        return (
            pltpu.make_async_copy(w.at[e], w_buf.at[slot], sem.at[slot, 0]),
            pltpu.make_async_copy(avg.at[e], avg_buf.at[slot], sem.at[slot, 1]),
        )

    def prime(m, start, stop):
        for i in range(min(SLOTS, stop - start)):
            for copy in loads(m, start + i, i):
                copy.start()

    def stream(m, start, stop, body):
        count = stop - start

        def step(i, carry):
            slot = lax.rem(i, SLOTS)
            for copy in loads(m, start + i, slot):
                copy.wait()
            body(start + i, slot)

            @pl.when(i + SLOTS < count)
            def _():
                for copy in loads(m, start + i + SLOTS, slot):
                    copy.start()

            return carry

        lax.fori_loop(0, count, step, 0)

    def column_sums(part, shift, e, slot):
        for k in range(n):
            at = slice(k * width, (k + 1) * width)
            fresh = fresh_of(wide_w[slot, :, at], wide_avg[slot, :, at])
            part[place_of(k, n), pl.ds(e + shift, 1), :] = jnp.sum(fresh * fresh, axis=0, keepdims=True)

    def row_sums(part, shift, e, slot):
        span = tall_w.shape[2]
        for k in range(n):
            at = slice(k * width, (k + 1) * width)
            total = None
            for c in range(span // LANES):
                lanes = slice(c * LANES, (c + 1) * LANES)
                fresh = fresh_of(tall_w[slot, at, lanes], tall_avg[slot, at, lanes])
                total = fresh * fresh if total is None else total + fresh * fresh
            part[place_of(k, n), pl.ds(e + shift, 1), :] = jnp.sum(total.T, axis=0, keepdims=True)

    def to_all(send):
        way = 2 * (me // half) - 1
        for d in range(1, n):
            send(lax.rem(me + way * d + n, n))

    def others(ref, sem, count=n - 1):
        some = ref.at[pl.ds(0, count)]
        return pltpu.make_async_copy(some, some, sem)

    def remote(src, dst, sent, arrived, k):
        return pltpu.make_async_remote_copy(
            src_ref=src, dst_ref=dst, send_sem=sent, recv_sem=arrived,
            device_id={"fsdp": k}, device_id_type=MESH,
        )

    def send_first():
        sums_a[me] = part_a[...]
        to_all(
            lambda k: remote(
                part_a, sums_a.at[me], sums_sent.at[0], sums_landed.at[0], k
            ).start()
        )

    def take_first():
        others(sums_a, sums_landed.at[0]).wait()

        def total(of):
            result = of(0)
            for k in range(1, n):
                result = result + of(k)
            return result

        scale_ref[0, 0:first] = jnp.sqrt(total(lambda k: sums_a[k, place]))
        inv_a[...] = 1.0 / jnp.sqrt(total(lambda k: sums_a[k]))

    def send_early():
        sums_b[me] = part_b[place]

        def send(k):
            remote(part_b.at[place_of(k, n)], sums_b.at[me], sums_sent.at[1], sums_landed.at[1], k).start()

        to_all(send)

    def keep_scale(scale, places):
        at = 0
        for m, start, stop in places:
            scale_ref[m, start:stop] = scale[at : at + stop - start]
            at += stop - start

    def send_early_inverse():
        others(sums_b, sums_landed.at[1]).wait()
        total = sums_b[0]
        for k in range(1, n):
            total = total + sums_b[k]
        scale = jnp.sqrt(total)
        keep_scale(scale, ((0, first, early),))
        inv_b[place] = 1.0 / scale
        to_all(
            lambda k: remote(
                inv_b.at[place], inv_b.at[place], inv_sent.at[1], inv_landed.at[1], k
            ).start()
        )

    def across(step):
        bit = chip // (1 << step) % 2
        return bit, (chip + (1 - 2 * bit) * (1 << step)) * 2 + core

    sibling = me + 1 - 2 * core
    theirs = pl.ds(pl.multiple_of((1 - core) * half, half), half)
    ours = pl.ds(pl.multiple_of(core * half, half), half)

    def send_rest():
        copy = remote(part_c.at[theirs], pair_c, pair_sent.at[0], pair_landed.at[0], sibling)
        copy.start()
        copy.wait_recv()
        part_c[ours] = part_c[ours] + pair_c[...]

    def halving(step):
        size = half >> (step + 1)
        base = core * half
        for before in range(step):
            base = base + across(before)[0] * (half >> (before + 1))
        bit, partner = across(step)
        keep, give = base + bit * size, base + (1 - bit) * size
        inbox = pl.ds(half - 2 * size, size)
        copy = remote(
            part_c.at[pl.ds(give, size)], sums_c.at[inbox],
            sums_sent.at[2 + step], sums_landed.at[2 + step], partner,
        )
        return copy, pl.ds(keep, size), inbox

    def send_half(step):
        halving(step)[0].start()

    def take_half(step):
        copy, keep, inbox = halving(step)
        copy.wait_recv()
        part_c[keep] = part_c[keep] + sums_c[inbox]

    def make_rest_inverse(places):
        scale = jnp.sqrt(part_c[place])
        keep_scale(scale, places)
        inv_c[place] = 1.0 / scale

    def doubling(step):
        size = half >> (step + 1)
        base = core * half
        for before in range(step + 1):
            base = base + across(before)[0] * (half >> (before + 1))
        some = inv_c.at[pl.ds(base, size)]
        return remote(
            some, some, inv_sent.at[2 + step], inv_landed.at[2 + step], across(step)[1]
        )

    def share_rest_inverse():
        copy = remote(inv_c.at[ours], inv_c.at[ours], pair_sent.at[1], pair_landed.at[1], sibling)
        copy.start()
        copy.wait_recv()

    def ring_slot(stage, sent, count):
        ring = lax.rem(count, RING)

        @pl.when(count >= RING)
        def _():
            others(stage.at[ring], sent.at[ring]).wait()

        return ring

    def wide_pieces(m, out, inv, shift, e, slot):
        ring = ring_slot(wide_stage, wide_sent, m * experts + e)
        for k in range(n):
            at = slice(k * width, (k + 1) * width)
            fresh = fresh_of(wide_w[slot, :, at], wide_avg[slot, :, at])
            wide_stage[ring, k] = (fresh * inv[place_of(k, n), pl.ds(e + shift, 1), :]).astype(jnp.bfloat16)
        rows = pl.ds(pl.multiple_of(me * depth, depth), depth)

        def send(k):
            pltpu.make_async_remote_copy(
                src_ref=wide_stage.at[ring, k], dst_ref=out.at[e, rows],
                send_sem=wide_sent.at[ring], recv_sem=landed.at[m, e],
                device_id={"fsdp": k}, device_id_type=MESH,
            ).start()

        to_all(send)
        out[e, rows] = wide_stage[ring, me]

    def tall_pieces(inv, shift, e, slot):
        ring = ring_slot(tall_stage, tall_sent, e)
        span = tall_w.shape[2]
        for k in range(n):
            at = slice(k * width, (k + 1) * width)
            row = inv[place_of(k, n), pl.ds(e + shift, 1), :]
            factor = jnp.broadcast_to(row, (LANES, width)).T
            for c in range(span // LANES):
                lanes = slice(c * LANES, (c + 1) * LANES)
                fresh = fresh_of(tall_w[slot, at, lanes], tall_avg[slot, at, lanes])
                tall_stage[ring, k, :, lanes] = (fresh * factor).astype(jnp.bfloat16)
        columns = pl.ds(pl.multiple_of(me * span, span), span)

        def send(k):
            pltpu.make_async_remote_copy(
                src_ref=tall_stage.at[ring, k], dst_ref=od_ref.at[e, :, columns],
                send_sem=tall_sent.at[ring], recv_sem=landed.at[2, e],
                device_id={"fsdp": k}, device_id_type=MESH,
            ).start()

        to_all(send)
        od_ref[e, :, columns] = tall_stage[ring, me]

    my_columns = pl.ds(pl.multiple_of(me * depth, depth), depth)

    def router_wait(sem):
        some = router_ref.at[group, :, pl.ds(0, (n - 1) * depth)]
        return pltpu.make_async_copy(some, some, sem)

    for e in range(first):
        for copy in loads(gate, e, SLOTS + e):
            copy.start()
    own_router[...] = (rw_ref[...] * gain_ref[...]).astype(jnp.bfloat16)
    router_ref[group, :, my_columns] = own_router[...]
    for e in range(first):
        for copy in loads(gate, e, SLOTS + e):
            copy.wait()
    prime(gate, first, early)
    for e in range(first):
        column_sums(part_a, 0, e, SLOTS + e)
    pl.semaphore_wait(barrier, n - 1 + ep - 1)
    send_first()
    stream(gate, first, early, functools.partial(column_sums, part_b, -first))
    send_early()
    to_all(
        lambda k: remote(
            own_router, router_ref.at[group, :, my_columns],
            router_sent.at[0], router_landed.at[0], k,
        ).start()
    )
    prime(gate, early, experts)
    prime(down, 0, experts)

    take_first()
    wide_pieces(0, og_ref, inv_a, 0, 0, SLOTS)
    send_early_inverse()
    for e in range(1, first):
        wide_pieces(0, og_ref, inv_a, 0, e, SLOTS + e)

    rest = experts - early
    stream(gate, early, experts, functools.partial(column_sums, part_c, -early))
    prime(up, 0, experts)
    stream(up, 0, experts, functools.partial(column_sums, part_c, rest))

    pieces_b = functools.partial(wide_pieces, 0, og_ref, inv_b, -first)
    cut_one = first + (early - first + 1) // 2
    prime(gate, first, cut_one)
    others(inv_b, inv_landed.at[1]).wait()
    stream(gate, first, cut_one, pieces_b)

    stream(down, 0, experts, functools.partial(row_sums, part_c, rest + experts))
    send_rest()
    turns = 2 * steps
    cuts = [cut_one + (early - cut_one) * i // max(1, turns) for i in range(turns + 1)]
    for step in range(steps):
        send_half(step)
        prime(gate, cuts[step], cuts[step + 1])
        stream(gate, cuts[step], cuts[step + 1], pieces_b)
        take_half(step)
    make_rest_inverse(((0, early, experts), (1, 0, experts), (2, 0, experts)))

    router_wait(router_landed.at[0]).wait()
    for d in range(1, ep):
        pltpu.make_async_remote_copy(
            src_ref=router_ref.at[group], dst_ref=router_ref.at[group],
            send_sem=router_sent.at[1], recv_sem=router_landed.at[1],
            device_id={"ep": lax.rem(group + d, ep)}, device_id_type=MESH,
        ).start()

    for turn, step in enumerate(reversed(range(steps)), steps):
        doubling(step).start()
        prime(gate, cuts[turn], cuts[turn + 1])
        stream(gate, cuts[turn], cuts[turn + 1], pieces_b)
        doubling(step).wait_recv()
    prime(gate, early, experts)
    prime(down, 0, experts)
    share_rest_inverse()
    stream(gate, early, experts, functools.partial(wide_pieces, 0, og_ref, inv_c, -early))
    prime(up, 0, experts)
    stream(up, 0, experts, functools.partial(wide_pieces, 1, ou_ref, inv_c, rest))
    stream(down, 0, experts, functools.partial(tall_pieces, inv_c, rest + experts))

    def arrived(m, e):
        stage = tall_stage if m == 2 else wide_stage
        others(stage.at[0], landed.at[m, e]).wait()

    def finish(m):
        def step(e, carry):
            arrived(m, e)
            return carry

        lax.fori_loop(0, experts, step, 0)

    def drain(count, stage, sent):
        def step(i, carry):
            others(stage.at[i], sent.at[i]).wait()
            return carry

        lax.fori_loop(0, min(RING, count), step, 0)

    others(sums_a, sums_sent.at[0]).wait()
    others(part_b, sums_sent.at[1]).wait()
    others(inv_b, inv_sent.at[1]).wait()
    for step in range(steps):
        halving(step)[0].wait_send()
        doubling(step).wait_send()
    others(pair_c, pair_sent.at[0], half).wait()
    others(inv_c, pair_sent.at[1], half).wait()
    router_wait(router_sent.at[0]).wait()
    if ep > 1:
        some = router_ref.at[pl.ds(0, ep - 1)]
        pltpu.make_async_copy(some, some, router_sent.at[1]).wait()
        pltpu.make_async_copy(some, some, router_landed.at[1]).wait()
    finish(0)
    finish(1)
    drain(2 * experts, wide_stage, wide_sent)
    drain(experts, tall_stage, tall_sent)
    finish(2)


def write_kernel(
    g_ref, u_ref, d_ref, scale_ref, router_ref,
    og_ref, ou_ref, od_ref, sg_ref, su_ref, sd_ref, out_router_ref, big, small,
):
    copies = []
    experts = g_ref.shape[0]
    parts = min(4, experts)
    span = experts // parts
    for m, (src, dst) in enumerate(((g_ref, og_ref), (u_ref, ou_ref), (d_ref, od_ref))):
        for i in range(parts):
            at = pl.ds(i * span, span)
            copies.append(pltpu.make_async_copy(src.at[at], dst.at[at], big.at[m, i]))
    for m, dst in enumerate((sg_ref, su_ref, sd_ref)):
        copies.append(pltpu.make_async_copy(scale_ref.at[m], dst, small.at[m]))
    copies.append(pltpu.make_async_copy(router_ref, out_router_ref, small.at[3]))
    for copy in copies:
        copy.start()
    for copy in copies:
        copy.wait()


def on_device(w_gate, avg_gate, w_up, avg_up, w_down, avg_down, router_weight, router_gain):
    n, ep = lax.axis_size("fsdp"), lax.axis_size("ep")
    experts, depth, d_expert = w_gate.shape
    span = w_down.shape[2]
    width = d_expert // n
    first, early = chunks_of(experts)
    rows = router_weight.shape[1]
    f32, bf16 = jnp.float32, jnp.bfloat16
    hbm = pl.BlockSpec(memory_space=pl.ANY)
    vmem = pl.BlockSpec(memory_space=pltpu.VMEM)
    shapes = (
        ((experts, n * depth, width), bf16),
        ((experts, n * depth, width), bf16),
        ((experts, width, n * span), bf16),
        ((3, experts, width), f32),
        ((ep, rows, n * depth), bf16),
    )
    counts = (first, early - first, 3 * experts - early)
    dma = pltpu.SemaphoreType.DMA
    work = pl.pallas_call(
        work_kernel,
        out_shape=[pltpu.VMEM(*shape) for shape in shapes],
        in_specs=[hbm] * 6 + [vmem] * 2,
        out_specs=[vmem] * 5,
        scratch_shapes=[
            pltpu.VMEM((SLOTS + first, depth, d_expert), f32),
            pltpu.VMEM((SLOTS + first, depth, d_expert), bf16),
            pltpu.VMEM((SLOTS, d_expert, span), f32),
            pltpu.VMEM((SLOTS, d_expert, span), bf16),
            pltpu.VMEM((RING, n, depth, width), bf16),
            pltpu.VMEM((RING, n, width, span), bf16),
            *[pltpu.VMEM((n, count, width), f32) for count in counts],
            pltpu.VMEM((n, n, first, width), f32),
            pltpu.VMEM((n, counts[1], width), f32),
            pltpu.VMEM((max(1, n // 2 - 1), counts[2], width), f32),
            *[pltpu.VMEM((n, count, width), f32) for count in counts],
            pltpu.VMEM((n // 2, counts[2], width), f32),
            pltpu.VMEM((rows, depth), bf16),
            dma((SLOTS + first, 2)),
            dma((SLOTS, 2)),
            dma((RING,)),
            dma((RING,)),
            dma((3, experts)),
            *[dma((2 + n.bit_length(),)) for _ in range(4)],
            *[dma((2,)) for _ in range(4)],
        ],
        compiler_params=pltpu.CompilerParams(
            collective_id=0, has_side_effects=True, vmem_limit_bytes=30 * MIB
        ),
    )
    results = work(
        w_gate, avg_gate, w_up, avg_up, w_down, avg_down,
        router_weight.T, router_gain.reshape(1, depth),
    )
    outs = (
        shapes[0],
        shapes[1],
        shapes[2],
        ((experts, width), f32),
        ((experts, width), f32),
        ((experts, width), f32),
        shapes[4],
    )
    write = pl.pallas_call(
        write_kernel,
        out_shape=[jax.ShapeDtypeStruct(*shape) for shape in outs],
        in_specs=[vmem] * 5,
        out_specs=[hbm] * 7,
        scratch_shapes=[dma((3, min(4, experts))), dma((4,))],
        compiler_params=pltpu.CompilerParams(vmem_limit_bytes=4 * MIB),
    )
    *arrays, router = write(*results)
    return (*arrays, router.reshape(ep * rows, n * depth).T)


def solution(mesh):
    placed = (
        P("ep", "fsdp", None),
        P("ep", "fsdp", None),
        P("ep", "fsdp", None),
        P("ep", "fsdp", None),
        P("ep", None, "fsdp"),
        P("ep", None, "fsdp"),
        P("fsdp", "ep"),
        P("fsdp"),
    )
    return jax.shard_map(
        on_device,
        mesh=mesh,
        in_specs=placed,
        out_specs=(
            P("ep", None, "fsdp"),
            P("ep", None, "fsdp"),
            P("ep", "fsdp", None),
            P("ep", "fsdp"),
            P("ep", "fsdp"),
            P("ep", "fsdp"),
            P(),
        ),
        check_vma=False,
    )
```
